32 devices in a mesh: rows: 4 (over y, x), feat: 8 (over z, core).
Axes of the slice: x: 2, y: 2, z: 4, core: 2. Of those that a mesh axis runs over, the one named last changes fastest.
Arguments:
- bins: int32 [256, 32768], P(None, ('rows', 'feat')), may hold values from 0 to 255
- leaf: int32 [32768], P(('rows', 'feat')), may hold values from 0 to 1
- grad: bfloat16 [32, 32768], P(None, ('rows', 'feat')), may hold values from -15.55 to 15.55
- hess: bfloat16 [32, 32768], P(None, ('rows', 'feat')), may hold values from 0.049804688 to 1
Outputs:
- gains: float32 [256, 2, 256], P(('rows', 'feat'))
- best: float32 [2], replicated
The draws below stay inside these ranges and needn't reach their ends.
All inputs are finite; a program needn't handle non-finite values.
Results may differ from the reference program's by a relative error of at most 0.0003.
Values may be sent and summed in bfloat16 or wider, within the bound.
A program may use at most 128 MiB of HBM per device.

```python
import math
import jax
import jax.numpy as jnp
from jax import lax

F = 256
B = 256
K = 32
LEAVES = 2
ROWS = 32768


def draw_grad(key, part):
    offset_key = jax.random.fold_in(key, 11)
    noise_key = jax.random.fold_in(key, 23)
    offset = jax.random.uniform(offset_key, (K, 1), jnp.float32, -0.25, 0.25)
    position = jnp.arange(ROWS, dtype=jnp.float32)[None, :] / max(ROWS - 1, 1)
    spread = 1.0 + 2.0 * position
    noise = jax.random.truncated_normal(noise_key, -4.0, 4.0, (K, ROWS), jnp.float32)
    return (offset + spread * noise).astype(jnp.bfloat16)


def plant(values, key, low, high):
    extent = values.shape
    spot = [jax.random.randint(jax.random.fold_in(key, axis), (), 0, extent[axis]) for axis in range(len(extent))]
    values = values.at[tuple(spot)].set(low)
    longest = extent.index(max(extent))
    spot[longest] = (spot[longest] + 1) % extent[longest]
    return values.at[tuple(spot)].set(high)


def levels(rng, shape, pieces, low, largest):
    factor_of = 1.0
    for dim, blocks in pieces:
        heights = jax.random.uniform(jax.random.fold_in(jax.random.fold_in(rng, 6), dim), (blocks,), jnp.float32, low / len(pieces), largest / len(pieces))
        factor_of = factor_of * jnp.repeat(jnp.exp(heights), shape[dim] // blocks).reshape((-1,) + (1,) * (len(shape) - 1 - dim))
    return factor_of


def setup_inputs(seed: int = 0) -> dict:
    key_of = jax.random.split(jax.random.key(seed), 5)
    bins = plant(jax.random.randint(key_of[0], (F, ROWS), 0, B), jax.random.fold_in(key_of[0], 1), 0, B - 1).astype(jnp.int32)
    leaf = plant(jax.random.randint(key_of[1], (ROWS,), 0, LEAVES), jax.random.fold_in(key_of[1], 1), 0, LEAVES - 1).astype(jnp.int32)
    grad = draw_grad(jax.random.fold_in(key_of[4], 71), 0)
    hess = jnp.clip(jnp.exp(math.log(1.0) - 2.9996462 * jax.random.uniform(key_of[3], (K, ROWS), jnp.float32) ** levels(key_of[3], (K, ROWS), ((1, 32),), -0.2, 0.2)), 0.049804688, 1.0).astype(jnp.bfloat16)
    return dict(bins=bins, leaf=leaf, grad=grad, hess=hess)


def split_gains(hist, totals):
    count = hist.shape[0]
    cum = jnp.cumsum(hist, axis=1).reshape(count, B, LEAVES, 2, K)
    tot = totals.reshape(LEAVES, 2, K)
    left_grad = cum[:, :, :, 0, :]
    left_hess = cum[:, :, :, 1, :]
    all_grad = tot[:, 0, :]
    all_hess = tot[:, 1, :]
    right_grad = all_grad - left_grad
    right_hess = all_hess - left_hess
    score = left_grad * left_grad / (left_hess + 1.0) + right_grad * right_grad / (right_hess + 1.0) - all_grad * all_grad / (all_hess + 1.0)
    gains = (0.5 / K) * jnp.sum(score, axis=-1)
    return jnp.transpose(gains, (0, 2, 1))


def reference(bins, leaf, grad, hess):
    both = jnp.concatenate([grad, hess], axis=0).astype(jnp.float32)
    nodes = jnp.arange(LEAVES, dtype=jnp.int32)
    hot = (leaf[None, :] == nodes[:, None]).astype(jnp.float32)
    weighted = (hot[:, None, :] * both[None, :, :]).reshape(LEAVES * 2 * K, ROWS).T

    def one_feature(codes):
        return jax.ops.segment_sum(weighted, codes, num_segments=B)

    hist = lax.map(one_feature, bins)
    totals = jnp.sum(weighted, axis=0)
    gains = split_gains(hist, totals)
    best = jnp.max(gains, axis=(0, 2))
    return gains, best
```

```python
import functools

import jax
import jax.numpy as jnp
from jax import lax
from jax.experimental import pallas as pl
from jax.experimental.pallas import tpu as pltpu
from jax.sharding import PartitionSpec as P

B = 256
LEAVES = 2
LANES = 128
MESH = pl.DeviceIdType.MESH


def add_block(codes, packed, acc_ref, outputs, shard):
    chunks = shard // LANES
    height = 2 * outputs
    both = jnp.concatenate([packed[j * height:(j + 1) * height, :] for j in range(chunks)], axis=1)
    start = chunks * height
    node = jnp.concatenate([packed[start + j:start + j + 1, :] for j in range(chunks)], axis=1)
    zero = jnp.zeros_like(both)
    weighted = jnp.concatenate([jnp.where(node == leaf, both, zero) for leaf in range(LEAVES)], axis=0)
    width = min(shard, 1024)
    levels = lax.broadcasted_iota(jnp.int32, (B, width), 0).astype(jnp.float32).astype(jnp.bfloat16)
    one = jnp.ones((B, width), jnp.bfloat16)
    none = jnp.zeros((B, width), jnp.bfloat16)
    for f in range(codes.shape[0]):
        total = acc_ref[f]
        for k in range(0, shard, width):
            upto = jnp.where(codes[f:f + 1, k:k + width] <= levels, one, none)
            total = total + lax.dot_general(
                weighted[:, k:k + width], upto, (((1,), (1,)), ((), ())), preferred_element_type=jnp.float32
            )
        acc_ref[f] = total


def feature_gains(cum, outputs):
    rows = []
    for leaf in range(LEAVES):
        base = leaf * 2 * outputs
        left_grad = cum[base:base + outputs]
        left_hess = cum[base + outputs:base + 2 * outputs]
        all_grad = left_grad[:, B - 1:B]
        all_hess = left_hess[:, B - 1:B]
        right_grad = all_grad - left_grad
        right_hess = all_hess - left_hess
        score = (
            left_grad * left_grad / (left_hess + 1.0)
            + right_grad * right_grad / (right_hess + 1.0)
            - all_grad * all_grad / (all_hess + 1.0)
        )
        rows.append(0.5 / outputs * jnp.sum(score, axis=0, keepdims=True))
    return jnp.concatenate(rows, axis=0)


def kernel(sizes, outputs, shard, owned, codes_in, packed_in, gains_ref, best_ref,
           codes_all, packed_all, acc_ref, best_all, send_c, recv_c, send_g, recv_g, send_b, recv_b):
    na, nb, nz = sizes
    pairs = na * nb * nz
    count = 2 * pairs
    r = lax.axis_index("rows")
    f = lax.axis_index("feat")
    a, b = r // nb, r % nb
    z, c = f // 2, f % 2

    def place(pa, pb, pz, pc):
        return {"rows": pa * nb + pb, "feat": pz * 2 + pc}

    def line(pa, pb, pz, pc):
        return ((pa * nb + pb) * nz + pz) * 2 + pc

    def digits(p):
        return p // (nb * nz), (p // nz) % nb, p % nz

    me = line(a, b, z, c)

    def source(p, pc):
        da, db, dz = digits(p)
        return line((a + da) % na, (b + db) % nb, (z + dz) % nz, pc)

    def target(s):
        da, db, dz = digits(s // 2)
        return (a + na - da) % na, (b + nb - db) % nb, (z + nz - dz) % nz, (c + s) % 2

    barrier = pltpu.get_barrier_semaphore()

    @pl.loop(1, count)
    def _(s):
        pl.semaphore_signal(barrier, inc=1, device_id=place(*target(s)), device_id_type=MESH)

    pl.semaphore_wait(barrier, count - 1)

    def packed_copy(src, slot, sem, where):
        return pltpu.make_async_remote_copy(
            src_ref=src, dst_ref=packed_all.at[slot], send_sem=send_g.at[sem], recv_sem=recv_g.at[slot],
            device_id=where, device_id_type=MESH)

    def codes_copy(s):
        where = target(s)
        return pltpu.make_async_remote_copy(
            src_ref=codes_in.at[line(*where)], dst_ref=codes_all.at[me], send_sem=send_c.at[s],
            recv_sem=recv_c.at[me], device_id=place(*where), device_id_type=MESH)

    def best_copy(s):
        return pltpu.make_async_remote_copy(
            src_ref=best_all.at[me], dst_ref=best_all.at[me], send_sem=send_b.at[s],
            recv_sem=recv_b.at[me], device_id=place(*target(s)), device_id_type=MESH)

    other = 1 - c
    for k in range(1, nz):
        packed_copy(packed_in, me, k, place(a, b, (z + nz - k) % nz, c)).start()
    packed_copy(packed_in, me, nz, place(a, (b + 1) % nb, z, c)).start()
    for k in range(1, na):
        packed_copy(packed_in, me, nb * nz * k, place((a + na - k) % na, b, z, c)).start()
    packed_copy(packed_in, me, nb * nz * na, place(a, b, z, other)).start()

    @pl.loop(1, count)
    def _(s):
        codes_copy(s).start()

    acc_ref[...] = jnp.zeros_like(acc_ref)
    packed_all[me] = packed_in[...]
    codes_all[me] = codes_in[me]

    @pl.loop(0, count)
    def _(s):
        p = s // 2
        here = source(p, (c + s) % 2)

        @pl.when(s > 0)
        def _():
            codes_copy_wait = pltpu.make_async_remote_copy(
                src_ref=codes_all.at[here], dst_ref=codes_all.at[here], send_sem=send_c.at[0],
                recv_sem=recv_c.at[here], device_id=place(a, b, z, other), device_id_type=MESH)
            codes_copy_wait.wait_recv()

        @pl.when(s % 2 == 1)
        def _():
            packed_copy(packed_in, here, 0, place(a, b, z, other)).wait_recv()

        add_block(codes_all[here], packed_all[here], acc_ref, outputs, shard)

        @pl.when(jnp.logical_and(s % 2 == 0, s + 2 < count))
        def _():
            q = p + 1
            slot = source(q, c)
            block = packed_all.at[slot]
            packed_copy(packed_in, slot, 0, place(a, b, z, other)).wait_recv()

            @pl.when(q < nb * nz)
            def _():
                for k in range(1, na):
                    packed_copy(block, slot, nb * nz * k + q, place((a + na - k) % na, b, z, c)).start()

            @pl.when(q < nz)
            def _():
                packed_copy(block, slot, nz + q, place(a, (b + 1) % nb, z, c)).start()

            packed_copy(block, slot, nb * nz * na + q, place(a, b, z, other)).start()

    top = None
    for i in range(owned):
        value = feature_gains(acc_ref[i], outputs)
        gains_ref[i] = value
        top = value if top is None else jnp.maximum(top, value)
    peak = jnp.max(top, axis=1, keepdims=True)
    lane = lax.broadcasted_iota(jnp.int32, (1, LANES), 1)
    best_all[me] = jnp.where(lane < LANES // 2, peak[0:1], peak[1:2])

    @pl.loop(1, count)
    def _(s):
        codes_copy(s).wait_send()
        packed_copy(packed_in, me, s, place(a, b, z, other)).wait_send()

    @pl.loop(1, count)
    def _(s):
        best_copy(s).start()

    @pl.loop(1, count)
    def _(s):
        here = source(s // 2, (c + s) % 2)
        pltpu.make_async_remote_copy(
            src_ref=best_all.at[here], dst_ref=best_all.at[here], send_sem=send_b.at[0],
            recv_sem=recv_b.at[here], device_id=place(a, b, z, other), device_id_type=MESH).wait_recv()

    @pl.loop(1, count)
    def _(s):
        best_copy(s).wait_send()

    best_ref[...] = jnp.max(best_all[...], axis=0)


def shards(sizes, bins, leaf, grad, hess):
    na, nb, nz = sizes
    count = na * nb * nz * 2
    outputs = grad.shape[0]
    features, shard = bins.shape
    owned = features // count
    chunks = shard // LANES
    codes = bins.astype(jnp.bfloat16).reshape(count, owned, shard)
    both = jnp.concatenate([grad, hess], axis=0).reshape(2 * outputs, chunks, LANES)
    both = jnp.transpose(both, (1, 0, 2)).reshape(chunks * 2 * outputs, LANES)
    node = leaf.astype(jnp.bfloat16).reshape(chunks, LANES)
    node = jnp.pad(node, ((0, -chunks % 16), (0, 0)))
    packed = jnp.concatenate([both, node], axis=0)
    dma = pltpu.SemaphoreType.DMA((count,))
    gains, best = pl.pallas_call(
        functools.partial(kernel, sizes, outputs, shard, owned),
        out_shape=(
            jax.ShapeDtypeStruct((owned, LEAVES, B), jnp.float32),
            jax.ShapeDtypeStruct((1, LANES), jnp.float32),
        ),
        in_specs=[pl.BlockSpec(memory_space=pltpu.VMEM)] * 2,
        out_specs=(pl.BlockSpec(memory_space=pltpu.VMEM),) * 2,
        scratch_shapes=[
            pltpu.VMEM(codes.shape, jnp.bfloat16),
            pltpu.VMEM((count,) + packed.shape, jnp.bfloat16),
            pltpu.VMEM((owned, LEAVES * 2 * outputs, B), jnp.float32),
            pltpu.VMEM((count, 1, LANES), jnp.float32),
            dma, dma, dma, dma, dma, dma,
        ],
        compiler_params=pltpu.CompilerParams(
            collective_id=0, has_side_effects=True, vmem_limit_bytes=56 * 1024 * 1024
        ),
    )(codes, packed)
    return gains, best[0, ::LANES // LEAVES]


def solution(mesh):
    rows, feat = mesh.shape["rows"], mesh.shape["feat"]
    sizes = (rows // 2, 2, feat // 2)
    return jax.shard_map(
        functools.partial(shards, sizes),
        mesh=mesh,
        in_specs=(
            P(None, ("rows", "feat")),
            P(("rows", "feat")),
            P(None, ("rows", "feat")),
            P(None, ("rows", "feat")),
        ),
        out_specs=(P(("rows", "feat"), None, None), P()),
        check_vma=False,
    )
```

```python
import functools

import jax
import jax.numpy as jnp
from jax import lax
from jax.experimental import pallas as pl
from jax.experimental.pallas import tpu as pltpu
from jax.sharding import PartitionSpec as P

B = 256
LEAVES = 2
LANES = 128
MESH = pl.DeviceIdType.MESH


def add_block(codes, packed, acc_ref, outputs, shard):
    chunks = shard // LANES
    height = 2 * outputs
    both = jnp.concatenate([packed[j * height:(j + 1) * height, :] for j in range(chunks)], axis=1)
    start = chunks * height
    node = jnp.concatenate([packed[start + j:start + j + 1, :] for j in range(chunks)], axis=1)
    zero = jnp.zeros_like(both)
    weighted = jnp.concatenate([jnp.where(node == leaf, both, zero) for leaf in range(LEAVES)], axis=0)
    columns = codes.astype(jnp.float32).T.astype(jnp.bfloat16)
    levels = lax.broadcasted_iota(jnp.int32, (shard, B), 1).astype(jnp.float32).astype(jnp.bfloat16)
    one = jnp.ones((shard, B), jnp.bfloat16)
    none = jnp.zeros((shard, B), jnp.bfloat16)
    for f in range(codes.shape[0]):
        code = jnp.broadcast_to(columns[:, f:f + 1], (shard, B))
        acc_ref[f] += jnp.dot(weighted, jnp.where(code <= levels, one, none), preferred_element_type=jnp.float32)


def feature_gains(cum, outputs):
    rows = []
    for leaf in range(LEAVES):
        base = leaf * 2 * outputs
        left_grad = cum[base:base + outputs]
        left_hess = cum[base + outputs:base + 2 * outputs]
        all_grad = left_grad[:, B - 1:B]
        all_hess = left_hess[:, B - 1:B]
        right_grad = all_grad - left_grad
        right_hess = all_hess - left_hess
        score = (
            left_grad * left_grad / (left_hess + 1.0)
            + right_grad * right_grad / (right_hess + 1.0)
            - all_grad * all_grad / (all_hess + 1.0)
        )
        rows.append(0.5 / outputs * jnp.sum(score, axis=0, keepdims=True))
    return jnp.concatenate(rows, axis=0)


def kernel(sizes, outputs, shard, owned, bins_ref, leaf_ref, grad_ref, hess_ref, gains_ref, best_ref,
           codes_in, codes_all, packed_all, acc_ref, best_all, send_c, recv_c, send_g, recv_g, send_b, recv_b):
    na, nb, nz = sizes
    pairs = na * nb * nz
    count = 2 * pairs
    r = lax.axis_index("rows")
    f = lax.axis_index("feat")
    a, b = r // nb, r % nb
    z, c = f // 2, f % 2

    group = na * nb

    def place(pa, pb, pz, pc):
        return {"rows": pa * nb + pb, "feat": pz * 2 + pc}

    def line(pa, pb, pz, pc):
        return ((pa * nb + pb) * nz + pz) * 2 + pc

    def toggled(dz):
        value, bit = 0, 1
        while bit < nz:
            value = value + (z // bit + dz // bit) % 2 * bit
            bit *= 2
        return value

    def offsets(p, pc):
        da = (1 - pc) * ((p // nb) % na) + pc * (p % na)
        db = (1 - pc) * (p % nb) + pc * ((p // na) % nb)
        return da, db, p // group

    me = line(a, b, z, c)
    other = 1 - c

    def source(p, pc):
        da, db, dz = offsets(p, pc)
        return line((a + da) % na, (b + db) % nb, toggled(dz), pc)

    def target(s):
        da, db, dz = offsets(s // 2, c)
        return (a + na - da) % na, (b + nb - db) % nb, toggled(dz), (c + s) % 2

    rows_size, feat_size = na * nb, nz * 2
    row_at = [lax.rem(r + i, rows_size) for i in range(rows_size)]
    feat_at = [lax.rem(f + i, feat_size) for i in range(feat_size)]
    others = [(i, j) for i in range(rows_size) for j in range(feat_size) if i + j > 0]

    barrier = pltpu.get_barrier_semaphore()
    for i, j in others:
        pl.semaphore_signal(
            barrier, inc=1, device_id={"rows": row_at[i], "feat": feat_at[j]}, device_id_type=MESH)

    chunks = shard // LANES
    own = packed_all.at[me]
    for j in range(chunks):
        part = slice(j * LANES, (j + 1) * LANES)
        own[2 * j * outputs:(2 * j + 1) * outputs] = grad_ref[:, part]
        own[(2 * j + 1) * outputs:(2 * j + 2) * outputs] = hess_ref[:, part]
    node = leaf_ref[...].astype(jnp.float32)
    node = jnp.concatenate([node, jnp.zeros((-chunks % 16, LANES), jnp.float32)], axis=0)
    own[2 * chunks * outputs:] = node.astype(jnp.bfloat16)
    codes_in[...] = bins_ref[...].astype(jnp.float32).astype(jnp.bfloat16).reshape(codes_in.shape)
    codes_all[me] = codes_in[me]
    acc_ref[...] = jnp.zeros_like(acc_ref)

    pl.semaphore_wait(barrier, count - 1)

    def packed_copy(src, slot, sem, where):
        return pltpu.make_async_remote_copy(
            src_ref=src, dst_ref=packed_all.at[slot], send_sem=send_g.at[sem], recv_sem=recv_g.at[slot],
            device_id=where, device_id_type=MESH)

    def codes_copy(s):
        where = target(s)
        return pltpu.make_async_remote_copy(
            src_ref=codes_in.at[line(*where)], dst_ref=codes_all.at[me], send_sem=send_c.at[s],
            recv_sem=recv_c.at[me], device_id=place(*where), device_id_type=MESH)

    def best_copy(i, j):
        return pltpu.make_async_remote_copy(
            src_ref=best_all.at[me], dst_ref=best_all.at[me], send_sem=send_b.at[i * feat_size + j],
            recv_sem=recv_b.at[me], device_id={"rows": row_at[i], "feat": feat_at[j]}, device_id_type=MESH)

    def forward(p, block, slot):
        for core in range(2):
            n1, n2 = (nb, na) if core == 0 else (na, nb)

            def spot(step, k):
                along_b = (step == 1) == (core == 0)
                if along_b:
                    return place(a, (b + nb - k) % nb, z, c)
                return place((a + na - k) % na, b, z, c)

            @pl.when(jnp.logical_and(c == core, (p // n1) % n2 == 0))
            def _():
                for k in range(1, n2):
                    sem = nz * n1 + (p // group * n1 + p % n1) * (n2 - 1) + k - 1
                    packed_copy(block, slot, sem, spot(2, k)).start()

            @pl.when(jnp.logical_and(c == core, p % group == 0))
            def _():
                for k in range(1, n1):
                    packed_copy(block, slot, nz + p // group * (n1 - 1) + k - 1, spot(1, k)).start()

        packed_copy(block, slot, nz * group + p, place(a, b, z, other)).start()

    def take(p):
        slot = source(p, c)
        packed_copy(own, slot, 0, place(a, b, z, other)).wait_recv()
        forward(p, packed_all.at[slot], slot)

    for k in range(1, nz):
        packed_copy(own, me, k, place(a, b, toggled(k), c)).start()
    forward(jnp.int32(0), own, me)

    @pl.loop(1, count)
    def _(s):
        codes_copy(s).start()

    @pl.loop(0, count)
    def _(s):
        p = s // 2
        here = source(p, (c + s) % 2)

        @pl.when(s > 0)
        def _():
            codes_copy_wait = pltpu.make_async_remote_copy(
                src_ref=codes_all.at[here], dst_ref=codes_all.at[here], send_sem=send_c.at[0],
                recv_sem=recv_c.at[here], device_id=place(a, b, z, other), device_id_type=MESH)
            codes_copy_wait.wait_recv()

        @pl.when(s % 2 == 1)
        def _():
            packed_copy(own, here, 0, place(a, b, z, other)).wait_recv()

        add_block(codes_all[here], packed_all[here], acc_ref, outputs, shard)

        @pl.when(jnp.logical_and(s % 2 == 0, jnp.logical_and((p + 1) % group > 0, s + 2 < count)))
        def _():
            take(p + 1)

        @pl.when(jnp.logical_and(s % 2 == 0, jnp.logical_and(p % group == 1, p // group + 1 < nz)))
        def _():
            take((p // group + 1) * group)

    top = None
    for i in range(owned):
        value = feature_gains(acc_ref[i], outputs)
        gains_ref[i] = value
        top = value if top is None else jnp.maximum(top, value)
    peak = jnp.max(top, axis=1, keepdims=True)
    lane = lax.broadcasted_iota(jnp.int32, (1, LANES), 1)
    best_all[me] = jnp.where(lane < LANES // 2, peak[0:1], peak[1:2])

    @pl.loop(1, count)
    def _(s):
        pltpu.make_async_remote_copy(
            src_ref=codes_in.at[0], dst_ref=codes_all.at[0], send_sem=send_c.at[s],
            recv_sem=recv_c.at[0], device_id=place(a, b, z, other), device_id_type=MESH).wait_send()
        packed_copy(own, me, s, place(a, b, z, other)).wait_send()

    for i, j in others:
        best_copy(i, j).start()

    @pl.loop(0, count)
    def _(here):
        @pl.when(here != me)
        def _():
            pltpu.make_async_remote_copy(
                src_ref=best_all.at[here], dst_ref=best_all.at[here], send_sem=send_b.at[0],
                recv_sem=recv_b.at[here], device_id=place(a, b, z, other), device_id_type=MESH).wait_recv()

    for i, j in others:
        best_copy(i, j).wait_send()

    best_ref[...] = jnp.max(best_all[...], axis=0)


def shards(sizes, bins, leaf, grad, hess):
    na, nb, nz = sizes
    count = na * nb * nz * 2
    outputs = grad.shape[0]
    features, shard = bins.shape
    owned = features // count
    chunks = shard // LANES
    packed_rows = chunks * 2 * outputs + chunks + -chunks % 16
    codes_shape = (count, owned, shard)
    dma = pltpu.SemaphoreType.DMA((count,))
    gains, best = pl.pallas_call(
        functools.partial(kernel, sizes, outputs, shard, owned),
        out_shape=(
            jax.ShapeDtypeStruct((owned, LEAVES, B), jnp.float32),
            jax.ShapeDtypeStruct((1, LANES), jnp.float32),
        ),
        in_specs=[pl.BlockSpec(memory_space=pltpu.VMEM)] * 4,
        out_specs=(pl.BlockSpec(memory_space=pltpu.VMEM),) * 2,
        scratch_shapes=[
            pltpu.VMEM(codes_shape, jnp.bfloat16),
            pltpu.VMEM(codes_shape, jnp.bfloat16),
            pltpu.VMEM((count, packed_rows, LANES), jnp.bfloat16),
            pltpu.VMEM((owned, LEAVES * 2 * outputs, B), jnp.float32),
            pltpu.VMEM((count, 1, LANES), jnp.float32),
            dma, dma, dma, dma, dma, dma,
        ],
        compiler_params=pltpu.CompilerParams(
            collective_id=0, has_side_effects=True, vmem_limit_bytes=56 * 1024 * 1024
        ),
    )(bins, leaf.reshape(chunks, LANES), grad, hess)
    return gains, best[0, ::LANES // LEAVES]


def solution(mesh):
    rows, feat = mesh.shape["rows"], mesh.shape["feat"]
    sizes = (rows // 2, 2, feat // 2)
    return jax.shard_map(
        functools.partial(shards, sizes),
        mesh=mesh,
        in_specs=(
            P(None, ("rows", "feat")),
            P(("rows", "feat")),
            P(None, ("rows", "feat")),
            P(None, ("rows", "feat")),
        ),
        out_specs=(P(("rows", "feat"), None, None), P()),
        check_vma=False,
    )
```

```python
import functools

import jax
import jax.numpy as jnp
from jax import lax
from jax.experimental import pallas as pl
from jax.experimental.pallas import tpu as pltpu
from jax.sharding import PartitionSpec as P

B = 256
LEAVES = 2
LANES = 128
MESH = pl.DeviceIdType.MESH


def add_block(codes, packed, acc_ref, outputs, shard):
    chunks = shard // LANES
    height = 2 * outputs
    both = jnp.concatenate([packed[j * height:(j + 1) * height, :] for j in range(chunks)], axis=1)
    start = chunks * height
    node = jnp.concatenate([packed[start + j:start + j + 1, :] for j in range(chunks)], axis=1)
    zero = jnp.zeros_like(both)
    weighted = jnp.concatenate([jnp.where(node == leaf, both, zero) for leaf in range(LEAVES)], axis=0)
    columns = codes.astype(jnp.float32).T.astype(jnp.bfloat16)
    levels = lax.broadcasted_iota(jnp.int32, (shard, B), 1).astype(jnp.float32).astype(jnp.bfloat16)
    one = jnp.ones((shard, B), jnp.bfloat16)
    none = jnp.zeros((shard, B), jnp.bfloat16)
    for f in range(codes.shape[0]):
        code = jnp.broadcast_to(columns[:, f:f + 1], (shard, B))
        acc_ref[f] += jnp.dot(weighted, jnp.where(code <= levels, one, none), preferred_element_type=jnp.float32)


def feature_gains(cum, outputs):
    rows = []
    for leaf in range(LEAVES):
        base = leaf * 2 * outputs
        left_grad = cum[base:base + outputs]
        left_hess = cum[base + outputs:base + 2 * outputs]
        all_grad = left_grad[:, B - 1:B]
        all_hess = left_hess[:, B - 1:B]
        right_grad = all_grad - left_grad
        right_hess = all_hess - left_hess
        score = (
            left_grad * left_grad / (left_hess + 1.0)
            + right_grad * right_grad / (right_hess + 1.0)
            - all_grad * all_grad / (all_hess + 1.0)
        )
        rows.append(0.5 / outputs * jnp.sum(score, axis=0, keepdims=True))
    return jnp.concatenate(rows, axis=0)


def kernel(sizes, outputs, shard, owned, bins_ref, leaf_ref, grad_ref, hess_ref, gains_ref, best_ref,
           codes_in, codes_all, packed_all, acc_ref, best_all, send_c, recv_c, send_g, recv_g, send_b, recv_b):
    na, nb, nz = sizes
    pairs = na * nb * nz
    count = 2 * pairs
    r = lax.axis_index("rows")
    f = lax.axis_index("feat")
    a, b = r // nb, r % nb
    z, c = f // 2, f % 2

    group = na * nb

    def place(pa, pb, pz, pc):
        return {"rows": pa * nb + pb, "feat": pz * 2 + pc}

    def line(pa, pb, pz, pc):
        return ((pa * nb + pb) * nz + pz) * 2 + pc

    def toggled(dz):
        value, bit = 0, 1
        while bit < nz:
            value = value + (z // bit + dz // bit) % 2 * bit
            bit *= 2
        return value

    def offsets(p, pc):
        da = (1 - pc) * ((p // nb) % na) + pc * (p % na)
        db = (1 - pc) * (p % nb) + pc * ((p // na) % nb)
        return da, db, p // group

    me = line(a, b, z, c)
    other = 1 - c

    def source(p, pc):
        da, db, dz = offsets(p, pc)
        return line((a + da) % na, (b + db) % nb, toggled(dz), pc)

    def target(s):
        da, db, dz = offsets(s // 2, c)
        return (a + na - da) % na, (b + nb - db) % nb, toggled(dz), (c + s) % 2

    rows_size, feat_size = na * nb, nz * 2
    row_at = [lax.rem(r + i, rows_size) for i in range(rows_size)]
    feat_at = [lax.rem(f + i, feat_size) for i in range(feat_size)]
    others = [(i, j) for i in range(rows_size) for j in range(feat_size) if i + j > 0]

    barrier = pltpu.get_barrier_semaphore()
    for i, j in others:
        pl.semaphore_signal(
            barrier, inc=1, device_id={"rows": row_at[i], "feat": feat_at[j]}, device_id_type=MESH)

    chunks = shard // LANES
    own = packed_all.at[me]
    for j in range(chunks):
        part = slice(j * LANES, (j + 1) * LANES)
        own[2 * j * outputs:(2 * j + 1) * outputs] = grad_ref[:, part]
        own[(2 * j + 1) * outputs:(2 * j + 2) * outputs] = hess_ref[:, part]
    node = leaf_ref[...].astype(jnp.float32)
    node = jnp.concatenate([node, jnp.zeros((-chunks % 16, LANES), jnp.float32)], axis=0)
    own[2 * chunks * outputs:] = node.astype(jnp.bfloat16)
    codes_in[...] = bins_ref[...].astype(jnp.float32).astype(jnp.bfloat16).reshape(codes_in.shape)
    codes_all[me] = codes_in[me]
    acc_ref[...] = jnp.zeros_like(acc_ref)

    pl.semaphore_wait(barrier, count - 1)

    def packed_copy(src, slot, sem, where):
        return pltpu.make_async_remote_copy(
            src_ref=src, dst_ref=packed_all.at[slot], send_sem=send_g.at[sem], recv_sem=recv_g.at[slot],
            device_id=where, device_id_type=MESH)

    def codes_copy(s):
        where = target(s)
        return pltpu.make_async_remote_copy(
            src_ref=codes_in.at[line(*where)], dst_ref=codes_all.at[me], send_sem=send_c.at[s],
            recv_sem=recv_c.at[me], device_id=place(*where), device_id_type=MESH)

    def best_copy(i, j):
        return pltpu.make_async_remote_copy(
            src_ref=best_all.at[me], dst_ref=best_all.at[me], send_sem=send_b.at[i * feat_size + j],
            recv_sem=recv_b.at[me], device_id={"rows": row_at[i], "feat": feat_at[j]}, device_id_type=MESH)

    def forward(p, block, slot):
        for core in range(2):
            n1, n2 = (nb, na) if core == 0 else (na, nb)

            def spot(step, k):
                along_b = (step == 1) == (core == 0)
                if along_b:
                    return place(a, (b + nb - k) % nb, z, c)
                return place((a + na - k) % na, b, z, c)

            @pl.when(jnp.logical_and(c == core, (p // n1) % n2 == 0))
            def _():
                for k in range(1, n2):
                    sem = nz * n1 + (p // group * n1 + p % n1) * (n2 - 1) + k - 1
                    packed_copy(block, slot, sem, spot(2, k)).start()

            @pl.when(jnp.logical_and(c == core, p % group == 0))
            def _():
                for k in range(1, n1):
                    packed_copy(block, slot, nz + p // group * (n1 - 1) + k - 1, spot(1, k)).start()

        packed_copy(block, slot, nz * group + p, place(a, b, z, other)).start()

    def take(p):
        slot = source(p, c)
        packed_copy(own, slot, 0, place(a, b, z, other)).wait_recv()
        forward(p, packed_all.at[slot], slot)

    for k in range(1, nz):
        packed_copy(own, me, k, place(a, b, toggled(k), c)).start()
    forward(jnp.int32(0), own, me)

    for s in range(1, count):
        codes_copy(s).start()

    @pl.loop(0, count)
    def _(s):
        p = s // 2
        here = source(p, (c + s) % 2)

        @pl.when(s > 0)
        def _():
            codes_copy_wait = pltpu.make_async_remote_copy(
                src_ref=codes_all.at[here], dst_ref=codes_all.at[here], send_sem=send_c.at[0],
                recv_sem=recv_c.at[here], device_id=place(a, b, z, other), device_id_type=MESH)
            codes_copy_wait.wait_recv()

        @pl.when(s % 2 == 1)
        def _():
            packed_copy(own, here, 0, place(a, b, z, other)).wait_recv()

        add_block(codes_all[here], packed_all[here], acc_ref, outputs, shard)

        @pl.when(jnp.logical_and(s % 2 == 0, jnp.logical_and((p + 1) % group > 0, s + 2 < count)))
        def _():
            take(p + 1)

        @pl.when(jnp.logical_and(s % 2 == 0, jnp.logical_and(p % group == 1, p // group + 1 < nz)))
        def _():
            take((p // group + 1) * group)

    top = None
    for i in range(owned):
        value = feature_gains(acc_ref[i], outputs)
        gains_ref[i] = value
        top = value if top is None else jnp.maximum(top, value)
    peak = jnp.max(top, axis=1, keepdims=True)
    lane = lax.broadcasted_iota(jnp.int32, (1, LANES), 1)
    best_all[me] = jnp.where(lane < LANES // 2, peak[0:1], peak[1:2])

    @pl.loop(1, count)
    def _(s):
        pltpu.make_async_remote_copy(
            src_ref=codes_in.at[0], dst_ref=codes_all.at[0], send_sem=send_c.at[s],
            recv_sem=recv_c.at[0], device_id=place(a, b, z, other), device_id_type=MESH).wait_send()
        packed_copy(own, me, s, place(a, b, z, other)).wait_send()

    for i, j in others:
        best_copy(i, j).start()

    @pl.loop(0, count)
    def _(here):
        @pl.when(here != me)
        def _():
            pltpu.make_async_remote_copy(
                src_ref=best_all.at[here], dst_ref=best_all.at[here], send_sem=send_b.at[0],
                recv_sem=recv_b.at[here], device_id=place(a, b, z, other), device_id_type=MESH).wait_recv()

    for i, j in others:
        best_copy(i, j).wait_send()

    best_ref[...] = jnp.max(best_all[...], axis=0)


def shards(sizes, bins, leaf, grad, hess):
    na, nb, nz = sizes
    count = na * nb * nz * 2
    outputs = grad.shape[0]
    features, shard = bins.shape
    owned = features // count
    chunks = shard // LANES
    packed_rows = chunks * 2 * outputs + chunks + -chunks % 16
    codes_shape = (count, owned, shard)
    dma = pltpu.SemaphoreType.DMA((count,))
    gains, best = pl.pallas_call(
        functools.partial(kernel, sizes, outputs, shard, owned),
        out_shape=(
            jax.ShapeDtypeStruct((owned, LEAVES, B), jnp.float32),
            jax.ShapeDtypeStruct((1, LANES), jnp.float32),
        ),
        in_specs=[pl.BlockSpec(memory_space=pltpu.VMEM)] * 4,
        out_specs=(pl.BlockSpec(memory_space=pltpu.VMEM),) * 2,
        scratch_shapes=[
            pltpu.VMEM(codes_shape, jnp.bfloat16),
            pltpu.VMEM(codes_shape, jnp.bfloat16),
            pltpu.VMEM((count, packed_rows, LANES), jnp.bfloat16),
            pltpu.VMEM((owned, LEAVES * 2 * outputs, B), jnp.float32),
            pltpu.VMEM((count, 1, LANES), jnp.float32),
            dma, dma, dma, dma, dma, dma,
        ],
        compiler_params=pltpu.CompilerParams(
            collective_id=0, has_side_effects=True, vmem_limit_bytes=56 * 1024 * 1024
        ),
    )(bins, leaf.reshape(chunks, LANES), grad, hess)
    return gains, best[0, ::LANES // LEAVES]


def solution(mesh):
    rows, feat = mesh.shape["rows"], mesh.shape["feat"]
    sizes = (rows // 2, 2, feat // 2)
    return jax.shard_map(
        functools.partial(shards, sizes),
        mesh=mesh,
        in_specs=(
            P(None, ("rows", "feat")),
            P(("rows", "feat")),
            P(None, ("rows", "feat")),
            P(None, ("rows", "feat")),
        ),
        out_specs=(P(("rows", "feat"), None, None), P()),
        check_vma=False,
    )
```
